256 devices in a mesh: groups: 2 (over z), seq: 128 (over x, y, core).
Axes of the slice: x: 8, y: 8, z: 2, core: 2. Of those that a mesh axis runs over, the one named last changes fastest.
The devices are a block of a 8x8x16 slice.
Arguments:
- query_rows: bfloat16 [131072, 1536], P(('groups', 'seq')), parts along dimension 0, may hold values from -200 to 200
- key_rows: bfloat16 [131072, 1536], P(('groups', 'seq')), parts along dimension 0, may hold values from -6 to 6
- value_rows: bfloat16 [131072, 1536], P(('groups', 'seq')), parts along dimension 0, may hold values from -6 to 6
- select: int32 [512, 6], P('groups'), parts along dimension 0, may hold values from 0 to 255, as said below
- counts: int32 [512], P('groups'), parts along dimension 0, may hold values from 2 to 6, as said below
- guide_scale: float32 [2], P('groups'), parts along dimension 0, may hold values from 4 to 8
Outputs:
- guided: bfloat16 [65536, 1536], P(('groups', 'seq')), parts along dimension 0
The draws below stay inside these ranges and needn't reach their ends.
There are 2 independent parts, one for each index of `groups`. The reference program is written for one: setup_inputs(seed, part) draws one part's arguments, and reference() takes and returns one part's arrays. A program takes and returns all parts, laid end to end along the dimension named above; each array names one. Nothing has to cross between parts.
Inputs may be any that keep to these rules, and one draw needn't show every extreme that they name: Row i begins with i itself. Its first counts[i] entries are distinct and name tiles of shards within 2 of tile i's shard, where tile t belongs to shard t // 4. The query tiles of one shard select at most 2 distinct tiles of any one other shard, and every shard selects 2 tiles of each shard within 2 in every draw. Entries past counts[i] are valid tile numbers that are not used. `counts`: whole shards are heavy or light, so the work of one device differs by about two times between devices.
All inputs are finite; a program needn't handle non-finite values.
Results may differ from the reference program's by a relative error of at most 0.0075.
Values may be sent and summed in bfloat16 or wider, within the bound.
No kernel may reach another device: no remote copies, remote signals or barrier semaphores. Data moves between devices by JAX's collectives and lax.ppermute only.
A program may use at most 128 MiB of HBM per device.

```python
import jax
import jax.numpy as jnp
from jax import lax

HEADS = 12
HEAD_DIM = 128
TILE = 128
TOK_DEV = 512
REACH = 2
CAP = 2
PICKS = 6
WIDTH = 1536
TILES_DEV = 4
SHARDS = 64
SEQLEN = 32768
NTILES = 256


def mask_tables(key):
    folded = jax.random.fold_in(key, 101)
    key_pool, key_score, key_heavy, key_count = jax.random.split(folded, 4)
    cand_count = TILES_DEV + 2 * REACH * CAP
    offset_list = jnp.array([moved for moved in range(-REACH, REACH + 1) if moved != 0], dtype=jnp.int32)
    shard_ids = jnp.arange(SHARDS, dtype=jnp.int32)
    tile_ids = jnp.arange(TILES_DEV, dtype=jnp.int32)
    pool_scores = jax.random.randint(key_pool, (SHARDS, 2 * REACH, TILES_DEV), 0, 1 << 16, dtype=jnp.int32) * TILES_DEV + tile_ids
    pool_local = lax.top_k(pool_scores, CAP)[1].astype(jnp.int32)
    owner_ids = shard_ids[:, None, None] + offset_list[None, :, None]
    pool_tiles = owner_ids * TILES_DEV + pool_local
    pool_valid = jnp.broadcast_to((owner_ids >= 0) & (owner_ids < SHARDS), pool_local.shape)
    local_tiles = shard_ids[:, None] * TILES_DEV + tile_ids[None, :]
    candidates = jnp.concatenate([local_tiles, pool_tiles.reshape(SHARDS, 2 * REACH * CAP)], axis=1)
    cand_valid = jnp.concatenate([jnp.ones((SHARDS, TILES_DEV), dtype=bool), pool_valid.reshape(SHARDS, 2 * REACH * CAP)], axis=1)
    cand_index = jnp.arange(cand_count, dtype=jnp.int32)
    noise_scores = jax.random.randint(key_score, (SHARDS, TILES_DEV, cand_count), 0, 1 << 16, dtype=jnp.int32) * cand_count + cand_index
    self_slot = cand_index[None, :] == tile_ids[:, None]
    block_index = (cand_index - TILES_DEV) // CAP
    row_of_block = (shard_ids[:, None] + block_index[None, :]) % TILES_DEV
    in_forced = (cand_index >= TILES_DEV)[None, None, :] & (tile_ids[None, :, None] == row_of_block[:, None, :])
    total_score = noise_scores + jnp.where(self_slot[None, :, :], 1 << 26, 0) + jnp.where(in_forced, 1 << 24, 0) - jnp.where(cand_valid[:, None, :], 0, 1 << 27)
    best_index = lax.top_k(total_score, PICKS)[1].astype(jnp.int32)
    spread = jnp.broadcast_to(candidates[:, None, :], (SHARDS, TILES_DEV, cand_count))
    select = jnp.take_along_axis(spread, best_index, axis=2).reshape(NTILES, PICKS).astype(jnp.int32)
    heavy_shard = jax.random.randint(key_heavy, (SHARDS,), 0, 4, dtype=jnp.int32) == 0
    many_picks = jax.random.randint(key_count, (SHARDS, TILES_DEV), PICKS - 2, PICKS + 1, dtype=jnp.int32)
    few_picks = jax.random.randint(jax.random.fold_in(key_count, 3), (SHARDS, TILES_DEV), 2, 4, dtype=jnp.int32)
    counts = jnp.where(heavy_shard[:, None], many_picks, few_picks)
    forced_row = (tile_ids[None, :] - shard_ids[:, None]) % TILES_DEV < 2 * REACH
    counts = jnp.where(forced_row, jnp.maximum(counts, CAP + 1), counts).reshape(NTILES).astype(jnp.int32)
    return (select, counts)


def draw_select(key, part):
    return mask_tables(key)[0]


def draw_counts(key, part):
    return mask_tables(key)[1]


def query_key_tables(key):
    folded = jax.random.fold_in(key, 202)
    key_query, key_key = jax.random.split(folded, 2)
    queries = jax.random.normal(key_query, (2 * SEQLEN, HEADS, HEAD_DIM), jnp.float32)
    keyset = jnp.clip(jax.random.normal(key_key, (2 * SEQLEN, HEADS, HEAD_DIM), jnp.float32), -6.0, 6.0)
    queries = jnp.clip(queries, -200.0, 200.0)
    return (queries.reshape(2 * SEQLEN, HEADS * HEAD_DIM), keyset.reshape(2 * SEQLEN, HEADS * HEAD_DIM))


def draw_query_rows(key, part):
    return query_key_tables(key)[0].astype(jnp.bfloat16)


def draw_key_rows(key, part):
    return query_key_tables(key)[1].astype(jnp.bfloat16)


def shard_levels(own_key, dims, cuts, low, largest):
    def one(dim, shards_of):
        draws = jax.random.uniform(jax.random.fold_in(jax.random.fold_in(own_key, 6), dim), (shards_of,), jnp.float32, low / len(cuts), largest / len(cuts))
        return jnp.repeat(jnp.exp(draws), dims[dim] // shards_of).reshape((-1,) + (1,) * (len(dims) - dim - 1))

    factor_of = one(*cuts[0])
    for cut in cuts[1:]:
        factor_of = factor_of * one(*cut)
    return factor_of


def scatter_about(own_key, dims, deviation, most, shards=(), kind=jnp.bfloat16):
    drawn = deviation * jax.random.normal(own_key, dims, jnp.float32)
    if shards:
        drawn = drawn * shard_levels(own_key, dims, shards, -0.22, 0.18)
    return jnp.clip(drawn, -most, most).astype(kind)


def setup_inputs(seed: int = 0, part: int = 0) -> dict:
    splits = jax.random.split(jax.random.key(seed), 7)
    own_keys = jax.random.split(jax.random.fold_in(splits[6], part), 7)
    query_rows = draw_query_rows(jax.random.fold_in(jax.random.fold_in(splits[6], part), 71), part)
    key_rows = draw_key_rows(jax.random.fold_in(jax.random.fold_in(splits[6], part), 71), part)
    value_rows = scatter_about(own_keys[2], (2 * SEQLEN, WIDTH), 1.0, 6.0, ((0, 128),))
    select = draw_select(jax.random.fold_in(jax.random.fold_in(splits[6], part), 71), part)
    counts = draw_counts(jax.random.fold_in(jax.random.fold_in(splits[6], part), 71), part)
    guide_scale = jnp.clip(jax.random.uniform(own_keys[5], (1,), jnp.float32, 4.0, 8.0), 4.0, 8.0)
    return {"query_rows": query_rows, "key_rows": key_rows, "value_rows": value_rows, "select": select, "counts": counts, "guide_scale": guide_scale}


def attend_tile(query_tile, key_sel, value_sel, alive_slots):
    score_scale = HEAD_DIM ** -0.5
    scores = jnp.einsum("thd,pshd->htps", query_tile.astype(jnp.float32), key_sel.astype(jnp.float32)) * score_scale
    scores = jnp.where(alive_slots[None, None, :, None], scores, -jnp.inf)
    row_max = jnp.max(scores, axis=(2, 3), keepdims=True)
    weights = jnp.exp(scores - row_max)
    denominator = jnp.sum(weights, axis=(2, 3))
    rounded = lax.optimization_barrier(weights.astype(jnp.bfloat16)).astype(jnp.float32)
    weighted = jnp.einsum("htps,pshd->thd", rounded, value_sel.astype(jnp.float32))
    return (weighted / jnp.transpose(denominator)[:, :, None]).astype(jnp.bfloat16)


def branch_major(rows, ntiles):
    split = rows.reshape(SHARDS, 2, TOK_DEV, HEADS * HEAD_DIM)
    return jnp.transpose(split, (1, 0, 2, 3)).reshape(2, ntiles, TILE, HEADS, HEAD_DIM)


def reference(query_rows, key_rows, value_rows, select, counts, guide_scale):
    ntiles = select.shape[0]
    query_tiles = branch_major(query_rows, ntiles)
    key_tiles = branch_major(key_rows, ntiles)
    value_tiles = branch_major(value_rows, ntiles)
    alive_all = jnp.arange(PICKS, dtype=jnp.int32)[None, :] < counts[:, None]
    guidance = guide_scale[0]

    def one_tile(inputs):
        cond_query, uncond_query, chosen, alive_slots = inputs
        cond_out = attend_tile(cond_query, key_tiles[0][chosen], value_tiles[0][chosen], alive_slots)
        uncond = attend_tile(uncond_query, key_tiles[1][chosen], value_tiles[1][chosen], alive_slots)
        cond_wide = lax.optimization_barrier(cond_out).astype(jnp.float32)
        uncond_wide = lax.optimization_barrier(uncond).astype(jnp.float32)
        mixed_out = uncond_wide + guidance * (cond_wide - uncond_wide)
        return mixed_out.astype(jnp.bfloat16).reshape(TILE, HEADS * HEAD_DIM)

    guided = lax.map(one_tile, (query_tiles[0], query_tiles[1], select, alive_all), batch_size=4)
    return guided.reshape(ntiles * TILE, HEADS * HEAD_DIM)
```

```python
import functools

import jax
import jax.numpy as jnp
from jax import lax
from jax.experimental import pallas as pl
from jax.experimental.pallas import tpu as pltpu
from jax.sharding import PartitionSpec as P

HEADS = 12
HEAD_DIM = 128
TILE = 128
REACH = 2
CAP = 2
OFFSETS = (-2, -1, 1, 2)
CHUNKS = (4, 4, 3, 1)
EXP2_SCALE = HEAD_DIM ** (-0.5) * 1.4426950408889634


def shifted(block, axis, distance):
    devices = range(lax.axis_size(axis))
    route = [(i - distance, i) for i in devices if i - distance in devices]
    return lax.ppermute(block, axis, route)


def partner(block, axis):
    route = [(i, i ^ 1) for i in range(lax.axis_size(axis))]
    return lax.ppermute(block, axis, route)


def first_bit(bits):
    return jnp.where(
        bits & 1 != 0, 0, jnp.where(bits & 2 != 0, 1, jnp.where(bits & 4 != 0, 2, 3))
    )


def wanted_bits(select, counts, shard, tiles_dev, picks):
    def one_row(row, bits):
        line = shard * tiles_dev + row
        live = counts[line]
        for pick in range(picks):
            place = select[line, pick] - (shard - REACH) * tiles_dev
            place = jnp.clip(place, 0, (2 * REACH + 1) * tiles_dev - 1)
            bits = bits | jnp.where(pick < live, jnp.left_shift(1, place), 0)
        return bits

    return lax.fori_loop(0, tiles_dev, one_row, jnp.int32(0))


def make_tables(me, select, counts, table, tiles_dev, picks, shards):
    my_shard = me // 2
    for index, offset in enumerate(OFFSETS):
        reader = jnp.clip(my_shard + offset, 0, shards - 1)
        bits = wanted_bits(select, counts, reader, tiles_dev, picks)
        mine = jnp.right_shift(bits, (REACH - offset) * tiles_dev) & 15
        table[2 * index] = first_bit(mine)
        table[2 * index + 1] = first_bit(mine & (mine - 1))
    bits = wanted_bits(select, counts, my_shard, tiles_dev, picks)

    def one_row(row, carry):
        line = my_shard * tiles_dev + row
        table[32 + row] = counts[line]
        for pick in range(picks):
            tile = select[line, pick]
            away = jnp.clip(tile // tiles_dev - my_shard, -REACH, REACH)
            within = tile % tiles_dev
            theirs = jnp.right_shift(bits, (away + REACH) * tiles_dev)
            below = theirs & (jnp.left_shift(1, within) - 1)
            rank = (below & 1) + (jnp.right_shift(below, 1) & 1) + (jnp.right_shift(below, 2) & 1)
            rank = jnp.minimum(rank, CAP - 1)
            block = jnp.where(away < 0, REACH - 1 - away, REACH - away)
            slot = jnp.where(away == 0, within, tiles_dev + block * CAP + rank)
            table[8 + row * picks + pick] = slot
        return carry

    lax.fori_loop(0, tiles_dev, one_row, 0)


def pack_copies(table, stage, outs, sems, begin):
    copies = []
    for index in range(len(OFFSETS)):
        for which in range(2):
            for slot in range(CAP):
                tile = table[2 * index + slot]
                copies.append(
                    pltpu.make_async_copy(
                        stage.at[which, pl.ds(pl.multiple_of(tile * TILE, TILE), TILE), :],
                        outs[index].at[which, pl.ds(slot * TILE, TILE), :],
                        sems.at[begin + (index * 2 + which) * CAP + slot],
                    )
                )
    return copies


def load_stage(keys, values, stage, sems, columns):
    loads = [
        pltpu.make_async_copy(keys.at[:, columns], stage.at[0], sems.at[0]),
        pltpu.make_async_copy(values.at[:, columns], stage.at[1], sems.at[1]),
    ]
    for load in loads:
        load.start()
    return loads


def first_pack_kernel(sizes, columns, me, select, counts, keys, values, table, *rest):
    outs, (stage, sems) = rest[:4], rest[4:]
    loads = load_stage(keys, values, stage, sems, columns)
    make_tables(me[0], select, counts, table, *sizes)
    for load in loads:
        load.wait()
    copies = pack_copies(table, stage, outs, sems, 2)
    for copy in copies:
        copy.start()
    for copy in copies:
        copy.wait()


def pack_kernel(begins, widths, table, keys, values, *rest):
    outs, (stage, sems) = rest[: 4 * len(begins)], rest[4 * len(begins) :]
    tokens, row_width = keys.shape
    loads = load_stage(keys, values, stage, sems, pl.ds(0, row_width))
    for load in loads:
        load.wait()
    copies = []
    per_chunk = len(OFFSETS) * 2 * CAP
    for index, (begin, width) in enumerate(zip(begins, widths)):
        part = stage.at[:, :, pl.ds(begin, width)]
        boxes = outs[4 * index : 4 * index + 4]
        copies += pack_copies(table, part, boxes, sems, 2 + per_chunk * index)
    for copy in copies:
        copy.start()
    for copy in copies:
        copy.wait()


def attend_tile(query_ref, pool, result, slots, rows, heads):
    live = len(slots)
    for head in heads:
        cols = slice(head * HEAD_DIM, (head + 1) * HEAD_DIM)
        query = query_ref[rows, cols]
        keys = jnp.concatenate([pool[0, slot, cols] for slot in slots], axis=0)
        values = jnp.concatenate([pool[1, slot, cols] for slot in slots], axis=0)
        scores = lax.dot_general(
            query, keys, (((1,), (1,)), ((), ())), preferred_element_type=jnp.float32
        )
        top = jnp.max(scores, axis=1, keepdims=True)
        weights = jnp.exp2((scores - top) * EXP2_SCALE)
        total = jnp.sum(weights, axis=1, keepdims=True)
        mixed = jnp.dot(weights.astype(jnp.bfloat16), values, preferred_element_type=jnp.float32)
        result[rows, cols] = (mixed / total).astype(jnp.bfloat16)


def attend_kernel(columns, heads, picks, half, table, queries, keys, values, *rest):
    lands, (sent, kept) = rest[:4], rest[4:6]
    query_ref, pool, result, sems = rest[6:]
    tokens = queries.shape[0]
    tiles_dev = tokens // TILE
    span = CAP * TILE
    copies = [
        pltpu.make_async_copy(queries.at[:, columns], query_ref, sems.at[0]),
        pltpu.make_async_copy(keys.at[:, columns], pool.at[0, pl.ds(0, tokens), :], sems.at[1]),
        pltpu.make_async_copy(values.at[:, columns], pool.at[1, pl.ds(0, tokens), :], sems.at[2]),
    ]
    for index, land in enumerate(lands):
        copies.append(
            pltpu.make_async_copy(
                land, pool.at[:, pl.ds(tokens + index * span, span), :], sems.at[3 + index]
            )
        )
    for copy in copies:
        copy.start()
    for copy in copies:
        copy.wait()

    def one_tile(tile, carry):
        rows = pl.ds(pl.multiple_of(tile * TILE, TILE), TILE)
        slots = [
            pl.ds(pl.multiple_of(table[8 + tile * picks + pick] * TILE, TILE), TILE)
            for pick in range(picks)
        ]
        live = table[32 + tile]
        for count in range(2, picks + 1):

            @pl.when(live == count)
            def _(count=count):
                attend_tile(query_ref, pool, result, slots[:count], rows, range(heads))

        return carry

    lax.fori_loop(0, tiles_dev, one_tile, 0)
    my_half = half[0]
    half_rows = tokens // 2
    outs = [
        pltpu.make_async_copy(
            result.at[pl.ds(pl.multiple_of((1 - my_half) * half_rows, half_rows), half_rows), :],
            sent,
            sems.at[7],
        ),
        pltpu.make_async_copy(
            result.at[pl.ds(pl.multiple_of(my_half * half_rows, half_rows), half_rows), :],
            kept,
            sems.at[8],
        ),
    ]
    for copy in outs:
        copy.start()
    for copy in outs:
        copy.wait()


def combine_kernel(half, guide, *rest):
    pieces, out = rest[:-1], rest[-1]
    count = len(pieces) // 2
    begin = 0
    conditional = half[0] == 0
    guidance = guide[0]
    for index in range(count):
        own = pieces[index][...].astype(jnp.float32)
        theirs = pieces[count + index][...].astype(jnp.float32)
        cond = jnp.where(conditional, own, theirs)
        uncond = jnp.where(conditional, theirs, own)
        width = own.shape[1]
        out[:, begin : begin + width] = (uncond + guidance * (cond - uncond)).astype(jnp.bfloat16)
        begin += width


SMEM = pl.BlockSpec(memory_space=pltpu.SMEM)
HBM = pl.BlockSpec(memory_space=pltpu.HBM)


def body(query_rows, key_rows, value_rows, select, counts, guide_scale):
    shards = lax.axis_size("seq") // 2
    me = lax.axis_index("seq").astype(jnp.int32)
    my_half = (me % 2).reshape(1)
    tokens, row_width = query_rows.shape
    tiles_dev = tokens // TILE
    picks = select.shape[1]
    half_rows = tokens // 2
    dtype = query_rows.dtype
    span = CAP * TILE

    begins = [sum(CHUNKS[:index]) * HEAD_DIM for index in range(len(CHUNKS))]
    widths = [heads * HEAD_DIM for heads in CHUNKS]

    def boxes_of(width):
        return [jax.ShapeDtypeStruct((2, span, width), dtype) for _ in OFFSETS]

    def scratch_of(width, chunks):
        return [
            pltpu.VMEM((2, tokens, width), dtype),
            pltpu.SemaphoreType.DMA((2 + chunks * len(OFFSETS) * 2 * CAP,)),
        ]

    def send(packed):
        return [shifted(box, "seq", 2 * offset) for box, offset in zip(packed, OFFSETS)]

    later = len(CHUNKS) - 1
    table, *packed = pl.pallas_call(
        functools.partial(
            first_pack_kernel, (tiles_dev, picks, shards), pl.ds(begins[0], widths[0])
        ),
        out_shape=[jax.ShapeDtypeStruct((64,), jnp.int32)] + boxes_of(widths[0]),
        in_specs=[SMEM, SMEM, SMEM, HBM, HBM],
        out_specs=[SMEM] + [HBM] * 4,
        scratch_shapes=scratch_of(widths[0], 1),
        name="pack_first",
    )(me.reshape(1), select, counts, key_rows, value_rows)
    landed = [send(packed)]
    packed = pl.pallas_call(
        functools.partial(pack_kernel, begins[1:], widths[1:]),
        out_shape=[box for width in widths[1:] for box in boxes_of(width)],
        in_specs=[SMEM, HBM, HBM],
        out_specs=[HBM] * (4 * later),
        scratch_shapes=scratch_of(row_width, later),
        name="pack_rest",
    )(table, key_rows, value_rows)
    landed += [send(packed[4 * index : 4 * index + 4]) for index in range(later)]

    kept_all, their_all = [], []
    for index, (begin, width, heads) in enumerate(zip(begins, widths, CHUNKS)):
        sent, kept = pl.pallas_call(
            functools.partial(attend_kernel, pl.ds(begin, width), heads, picks),
            out_shape=[jax.ShapeDtypeStruct((half_rows, width), dtype)] * 2,
            in_specs=[SMEM, SMEM] + [HBM] * 7,
            out_specs=[HBM, HBM],
            scratch_shapes=[
                pltpu.VMEM((tokens, width), dtype),
                pltpu.VMEM((2, tokens + len(OFFSETS) * span, width), dtype),
                pltpu.VMEM((tokens, width), dtype),
                pltpu.SemaphoreType.DMA((9,)),
            ],
            name=f"attend_{index}",
        )(my_half, table, query_rows, key_rows, value_rows, *landed[index])
        kept_all.append(kept)
        their_all.append(partner(sent, "seq"))
    return pl.pallas_call(
        combine_kernel,
        out_shape=jax.ShapeDtypeStruct((half_rows, row_width), dtype),
        in_specs=[SMEM, SMEM] + [pl.BlockSpec(memory_space=pltpu.VMEM)] * (2 * len(CHUNKS)),
        out_specs=pl.BlockSpec(memory_space=pltpu.VMEM),
        name="combine",
    )(my_half, guide_scale, *kept_all, *their_all)


def solution(mesh):
    in_specs = (
        P(("groups", "seq"), None),
        P(("groups", "seq"), None),
        P(("groups", "seq"), None),
        P("groups", None),
        P("groups"),
        P("groups"),
    )
    out_specs = P(("groups", "seq"), None)
    return jax.shard_map(body, mesh=mesh, in_specs=in_specs, out_specs=out_specs, check_vma=False)
```

```python
import functools

import jax
import jax.numpy as jnp
from jax import lax
from jax.experimental import pallas as pl
from jax.experimental.pallas import tpu as pltpu
from jax.sharding import PartitionSpec as P

HEAD_DIM = 128
TILE = 128
REACH = 2
CAP = 2
OFFSETS = (1, 2, -1, -2)
CHUNKS = (5, 4, 2, 1)
EXP2_SCALE = HEAD_DIM ** (-0.5) * 1.4426950408889634
VMEM_BYTES = 24 << 20


SMEM = pl.BlockSpec(memory_space=pltpu.SMEM)
VMEM = pl.BlockSpec(memory_space=pltpu.VMEM)
HBM = pl.BlockSpec(memory_space=pltpu.HBM)
PARAMS = pltpu.CompilerParams(vmem_limit_bytes=VMEM_BYTES)


def shifted(block, axis, distance):
    devices = range(lax.axis_size(axis))
    route = [(i - distance, i) for i in devices if i - distance in devices]
    return lax.ppermute(block, axis, route)


def partner(block, axis):
    route = [(i, i ^ 1) for i in range(lax.axis_size(axis))]
    return lax.ppermute(block, axis, route)


def first_bit(bits):
    return jnp.where(
        bits & 1 != 0, 0, jnp.where(bits & 2 != 0, 1, jnp.where(bits & 4 != 0, 2, 3))
    )


def wanted_bits(select, counts, shard, tiles_dev, picks):
    bits = jnp.int32(0)
    base = (shard - REACH) * tiles_dev
    for row in range(tiles_dev):
        line = shard * tiles_dev + row
        live = counts[line]
        for pick in range(picks):
            place = jnp.clip(select[pick, line] - base, 0, (2 * REACH + 1) * tiles_dev - 1)
            bits = bits | jnp.where(pick < live, jnp.left_shift(1, place), 0)
    return bits


def fill_slots(my_shard, select, counts, table, tiles_dev, picks):
    bits = wanted_bits(select, counts, my_shard, tiles_dev, picks)
    for row in range(tiles_dev):
        line = my_shard * tiles_dev + row
        table[tiles_dev * picks + row] = counts[line]
        for pick in range(picks):
            tile = select[pick, line]
            away = jnp.clip(tile // tiles_dev - my_shard, -REACH, REACH)
            within = tile % tiles_dev
            theirs = jnp.right_shift(bits, (away + REACH) * tiles_dev)
            below = theirs & (jnp.left_shift(1, within) - 1)
            rank = (below & 1) + (jnp.right_shift(below, 1) & 1) + (jnp.right_shift(below, 2) & 1)
            rank = jnp.minimum(rank, CAP - 1)
            block = jnp.where(away < 0, -away - 1, away + REACH - 1)
            slot = jnp.where(away == 0, within, tiles_dev + block * CAP + rank)
            table[row * picks + pick] = slot


def pack_kernel(sizes, begins, widths, me, select, counts, keys, values, table, *rest):
    tiles_dev, picks, shards = sizes
    outs, (stage, sems) = rest[:-2], rest[-2:]
    loads = [
        pltpu.make_async_copy(keys, stage.at[0], sems.at[0]),
        pltpu.make_async_copy(values, stage.at[1], sems.at[1]),
    ]
    for load in loads:
        load.start()
    my_shard = me[0] // 2
    tiles = []
    for offset in OFFSETS:
        reader = jnp.clip(my_shard + offset, 0, shards - 1)
        bits = wanted_bits(select, counts, reader, tiles_dev, picks)
        mine = jnp.right_shift(bits, (REACH - offset) * tiles_dev) & 15
        tiles.append((first_bit(mine), first_bit(mine & (mine - 1))))
    fill_slots(my_shard, select, counts, table, tiles_dev, picks)
    for load in loads:
        load.wait()
    for index, (begin, width) in enumerate(zip(begins, widths)):
        for place in range(len(OFFSETS)):
            out = outs[index * len(OFFSETS) + place]
            for which in range(2):
                for slot in range(CAP):
                    rows = pl.ds(pl.multiple_of(tiles[place][slot] * TILE, TILE), TILE)
                    out[which, slot * TILE : (slot + 1) * TILE, :] = stage[
                        which, rows, begin : begin + width
                    ]


def attend_tile(queries, pool, result, slots, rows, begin, heads):
    for head in heads:
        cols = slice(head * HEAD_DIM, (head + 1) * HEAD_DIM)
        query = queries[rows, begin + head * HEAD_DIM : begin + (head + 1) * HEAD_DIM]
        keys = jnp.concatenate([pool[0, slot, cols] for slot in slots], axis=0)
        values = jnp.concatenate([pool[1, slot, cols] for slot in slots], axis=0)
        scores = lax.dot_general(
            query, keys, (((1,), (1,)), ((), ())), preferred_element_type=jnp.float32
        )
        top = jnp.max(scores, axis=1, keepdims=True)
        weights = jnp.exp2((scores - top) * EXP2_SCALE)
        total = jnp.sum(weights, axis=1, keepdims=True)
        mixed = jnp.dot(weights.astype(jnp.bfloat16), values, preferred_element_type=jnp.float32)
        result[rows, cols] = (mixed / total).astype(jnp.bfloat16)


def attend_kernel(begin, heads, picks, half, table, queries, keys, values, *rest):
    lands, (sent, kept, pool, result) = rest[:4], rest[4:]
    tokens = queries.shape[0]
    tiles_dev = tokens // TILE
    span = CAP * TILE
    width = heads * HEAD_DIM
    pool[0, :tokens, :] = keys[:, begin : begin + width]
    pool[1, :tokens, :] = values[:, begin : begin + width]
    for index, land in enumerate(lands):
        pool[:, tokens + index * span : tokens + (index + 1) * span, :] = land[...]

    def one_tile(tile, carry):
        rows = pl.ds(pl.multiple_of(tile * TILE, TILE), TILE)
        slots = [
            pl.ds(pl.multiple_of(table[tile * picks + pick] * TILE, TILE), TILE)
            for pick in range(picks)
        ]
        live = table[tiles_dev * picks + tile]
        for count in range(2, picks + 1):

            @pl.when(live == count)
            def _(count=count):
                attend_tile(queries, pool, result, slots[:count], rows, begin, range(heads))

        return carry

    lax.fori_loop(0, tiles_dev, one_tile, 0)
    half_rows = tokens // 2
    my_half = half[0]
    sent[...] = result[pl.ds(pl.multiple_of((1 - my_half) * half_rows, half_rows), half_rows), :]
    kept[...] = result[pl.ds(pl.multiple_of(my_half * half_rows, half_rows), half_rows), :]


def combine_kernel(begin, count, aliased, half, guide, *rest):
    pieces, rest = rest[: 2 * count], rest[2 * count + aliased :]
    out, mixed, sem = rest
    conditional = half[0] == 0
    guidance = guide[0]
    at = 0
    for index in range(count):
        own = pieces[index][...].astype(jnp.float32)
        theirs = pieces[count + index][...].astype(jnp.float32)
        cond = jnp.where(conditional, own, theirs)
        uncond = jnp.where(conditional, theirs, own)
        width = own.shape[1]
        mixed[:, at : at + width] = (uncond + guidance * (cond - uncond)).astype(jnp.bfloat16)
        at += width
    copy = pltpu.make_async_copy(mixed, out.at[:, pl.ds(begin, at)], sem)
    copy.start()
    copy.wait()


def body(query_rows, key_rows, value_rows, select, counts, guide_scale):
    shards = lax.axis_size("seq") // 2
    me = lax.axis_index("seq").astype(jnp.int32)
    my_half = (me % 2).reshape(1)
    tokens, row_width = query_rows.shape
    tiles_dev = tokens // TILE
    picks = select.shape[1]
    half_rows = tokens // 2
    dtype = query_rows.dtype
    span = CAP * TILE
    chunks = len(CHUNKS)
    begins = [sum(CHUNKS[:index]) * HEAD_DIM for index in range(chunks)]
    widths = [heads * HEAD_DIM for heads in CHUNKS]

    table, *packed = pl.pallas_call(
        functools.partial(pack_kernel, (tiles_dev, picks, shards), begins, widths),
        out_shape=[jax.ShapeDtypeStruct((tiles_dev * (picks + 1),), jnp.int32)]
        + [jax.ShapeDtypeStruct((2, span, width), dtype) for width in widths for _ in OFFSETS],
        in_specs=[SMEM, SMEM, SMEM, HBM, HBM],
        out_specs=[SMEM] + [VMEM] * (chunks * len(OFFSETS)),
        scratch_shapes=[pltpu.VMEM((2, tokens, row_width), dtype), pltpu.SemaphoreType.DMA((2,))],
        compiler_params=PARAMS,
        name="pack",
    )(me.reshape(1), select.T, counts, key_rows, value_rows)

    landed = []
    for index in range(chunks):
        boxes = packed[len(OFFSETS) * index : len(OFFSETS) * (index + 1)]
        landed.append([shifted(box, "seq", 2 * off) for box, off in zip(boxes, OFFSETS)])

    kept_all, their_all = [], []
    for index, (begin, width, heads) in enumerate(zip(begins, widths, CHUNKS)):
        sent, kept = pl.pallas_call(
            functools.partial(attend_kernel, begin, heads, picks),
            out_shape=[jax.ShapeDtypeStruct((half_rows, width), dtype)] * 2,
            in_specs=[SMEM, SMEM] + [VMEM] * 7,
            out_specs=[VMEM, VMEM],
            scratch_shapes=[
                pltpu.VMEM((2, tokens + len(OFFSETS) * span, width), dtype),
                pltpu.VMEM((tokens, width), dtype),
            ],
            compiler_params=PARAMS,
        )(my_half, table, query_rows, key_rows, value_rows, *landed[index])
        kept_all.append(kept)
        their_all.append(partner(sent, "seq"))

    early = chunks - 1
    guided = None
    for first, last in ((0, early), (early, chunks)):
        pieces = kept_all[first:last] + their_all[first:last]
        aliased = [] if guided is None else [guided]
        guided = pl.pallas_call(
            functools.partial(combine_kernel, begins[first], last - first, len(aliased)),
            out_shape=jax.ShapeDtypeStruct((half_rows, row_width), dtype),
            in_specs=[SMEM, SMEM] + [VMEM] * len(pieces) + [HBM] * len(aliased),
            out_specs=HBM,
            scratch_shapes=[
                pltpu.VMEM((half_rows, sum(widths[first:last])), dtype),
                pltpu.SemaphoreType.DMA,
            ],
            input_output_aliases={2 + len(pieces): 0} if aliased else {},
            compiler_params=PARAMS,
        )(my_half, guide_scale, *pieces, *aliased)
    return guided


def solution(mesh):
    in_specs = (
        P(("groups", "seq"), None),
        P(("groups", "seq"), None),
        P(("groups", "seq"), None),
        P("groups", None),
        P("groups"),
        P("groups"),
    )
    out_specs = P(("groups", "seq"), None)

    return jax.shard_map(body, mesh=mesh, in_specs=in_specs, out_specs=out_specs, check_vma=False)
```

```python
import functools

import jax
import jax.numpy as jnp
from jax import lax
from jax.experimental import pallas as pl
from jax.experimental.pallas import tpu as pltpu
from jax.sharding import PartitionSpec as P

HEAD_DIM = 128
TILE = 128
REACH = 2
CAP = 2
OFFSETS = (1, -1, 2, -2)
NEAR = 2
CHUNKS = (6, 5, 1)
EXP2_SCALE = HEAD_DIM ** (-0.5) * 1.4426950408889634
VMEM_BYTES = 24 << 20


SMEM = pl.BlockSpec(memory_space=pltpu.SMEM)
VMEM = pl.BlockSpec(memory_space=pltpu.VMEM)
HBM = pl.BlockSpec(memory_space=pltpu.HBM)
PARAMS = pltpu.CompilerParams(vmem_limit_bytes=VMEM_BYTES)


def shifted(block, axis, distance):
    devices = range(lax.axis_size(axis))
    route = [(i - distance, i) for i in devices if i - distance in devices]
    return lax.ppermute(block, axis, route)


def partner(block, axis):
    route = [(i, i ^ 1) for i in range(lax.axis_size(axis))]
    return lax.ppermute(block, axis, route)


def first_bit(bits):
    return jnp.where(
        bits & 1 != 0, 0, jnp.where(bits & 2 != 0, 1, jnp.where(bits & 4 != 0, 2, 3))
    )


def wanted_bits(select, counts, shard, tiles_dev, picks):
    bits = jnp.int32(0)
    base = (shard - REACH) * tiles_dev
    for row in range(tiles_dev):
        line = shard * tiles_dev + row
        live = counts[line]
        for pick in range(picks):
            place = jnp.clip(select[pick, line] - base, 0, (2 * REACH + 1) * tiles_dev - 1)
            bits = bits | jnp.where(pick < live, jnp.left_shift(1, place), 0)
    return bits


def fill_table(my_shard, tiles, select, counts, table, tiles_dev, picks):
    bits = wanted_bits(select, counts, my_shard, tiles_dev, picks)
    for row in range(tiles_dev):
        line = my_shard * tiles_dev + row
        table[tiles_dev * picks + row] = counts[line]
        for pick in range(picks):
            tile = select[pick, line]
            away = jnp.clip(tile // tiles_dev - my_shard, -REACH, REACH)
            within = tile % tiles_dev
            theirs = jnp.right_shift(bits, (away + REACH) * tiles_dev)
            below = theirs & (jnp.left_shift(1, within) - 1)
            rank = (below & 1) + (jnp.right_shift(below, 1) & 1) + (jnp.right_shift(below, 2) & 1)
            rank = jnp.minimum(rank, CAP - 1)
            block = 2 * (jnp.abs(away) - 1) + jnp.where(away < 0, 0, 1)
            slot = jnp.where(away == 0, within, tiles_dev + block * CAP + rank)
            table[row * picks + pick] = slot
    for index, tile in enumerate(tiles):
        table[tiles_dev * (picks + 1) + index] = tile


def sent_tiles(my_shard, offset, select, counts, tiles_dev, picks, shards):
    reader = jnp.clip(my_shard + offset, 0, shards - 1)
    bits = wanted_bits(select, counts, reader, tiles_dev, picks)
    mine = jnp.right_shift(bits, (REACH - offset) * tiles_dev) & 15
    return [first_bit(mine), first_bit(mine & (mine - 1))]


def tile_rows(tile):
    return pl.ds(pl.multiple_of(tile * TILE, TILE), TILE)


def pack_near_kernel(sizes, me, select, counts, keys, values, table, *rest):
    outs, (stage, load_sems, sems) = rest[:NEAR], rest[NEAR:]
    my_shard = me[0] // 2
    loads = []
    for which, rows in enumerate((keys, values)):
        for tile in range(sizes[0]):
            part = pl.ds(tile * TILE, TILE)
            loads.append(
                pltpu.make_async_copy(
                    rows.at[part, :], stage.at[which, part, :], load_sems.at[len(loads)]
                )
            )
    for load in loads:
        load.start()
    near = [sent_tiles(my_shard, off, select, counts, *sizes) for off in OFFSETS[:NEAR]]
    for load in loads:
        load.wait()
    copies = []
    for index, chosen in enumerate(near):
        for slot, tile in enumerate(chosen):
            for which in range(2):
                copy = pltpu.make_async_copy(
                    stage.at[which, tile_rows(tile), :],
                    outs[index].at[which, pl.ds(slot * TILE, TILE), :],
                    sems.at[len(copies)],
                )
                copy.start()
                copies.append(copy)
    tiles = []
    for offset in OFFSETS[NEAR:]:
        tiles += sent_tiles(my_shard, offset, select, counts, *sizes)
    fill_table(my_shard, tiles, select, counts, table, *sizes[:2])
    for copy in copies:
        copy.wait()


def pack_far_kernel(first, begins, widths, table, keys, values, *outs):
    far = len(OFFSETS) - NEAR
    for index, (begin, width) in enumerate(zip(begins, widths)):
        for place in range(far):
            out = outs[index * far + place]
            for slot in range(CAP):
                rows = tile_rows(table[first + place * CAP + slot])
                for which, source in enumerate((keys, values)):
                    out[which, slot * TILE : (slot + 1) * TILE, :] = source[
                        rows, begin : begin + width
                    ]


def attend_tile(queries, pool, result, slots, rows, begin, heads):
    for head in heads:
        cols = slice(head * HEAD_DIM, (head + 1) * HEAD_DIM)
        query = queries[rows, begin + head * HEAD_DIM : begin + (head + 1) * HEAD_DIM]
        keys = jnp.concatenate([pool[0, slot, cols] for slot in slots], axis=0)
        values = jnp.concatenate([pool[1, slot, cols] for slot in slots], axis=0)
        scores = lax.dot_general(
            query, keys, (((1,), (1,)), ((), ())), preferred_element_type=jnp.float32
        )
        top = jnp.max(scores, axis=1, keepdims=True)
        weights = jnp.exp2((scores - top) * EXP2_SCALE)
        total = jnp.sum(weights, axis=1, keepdims=True)
        mixed = jnp.dot(weights.astype(jnp.bfloat16), values, preferred_element_type=jnp.float32)
        result[rows, cols] = (mixed / total).astype(jnp.bfloat16)


def attend_kernel(begin, heads, picks, half, table, queries, keys, values, *rest):
    lands, (sent, kept, pool, result) = rest[:4], rest[4:]
    tokens = queries.shape[0]
    tiles_dev = tokens // TILE
    span = CAP * TILE
    width = heads * HEAD_DIM
    pool[0, :tokens, :] = keys[:, begin : begin + width]
    pool[1, :tokens, :] = values[:, begin : begin + width]
    for index, land in enumerate(lands):
        at = begin if index < NEAR else 0
        pool[:, tokens + index * span : tokens + (index + 1) * span, :] = land[
            :, :, at : at + width
        ]

    def one_tile(tile, carry):
        rows = pl.ds(pl.multiple_of(tile * TILE, TILE), TILE)
        slots = [
            pl.ds(pl.multiple_of(table[tile * picks + pick] * TILE, TILE), TILE)
            for pick in range(picks)
        ]
        live = table[tiles_dev * picks + tile]
        for count in range(2, picks + 1):

            @pl.when(live == count)
            def _(count=count):
                attend_tile(queries, pool, result, slots[:count], rows, begin, range(heads))

        return carry

    lax.fori_loop(0, tiles_dev, one_tile, 0)
    half_rows = tokens // 2
    my_half = half[0]
    sent[...] = result[pl.ds(pl.multiple_of((1 - my_half) * half_rows, half_rows), half_rows), :]
    kept[...] = result[pl.ds(pl.multiple_of(my_half * half_rows, half_rows), half_rows), :]


def combine_kernel(begin, count, aliased, half, guide, *rest):
    pieces, rest = rest[: 2 * count], rest[2 * count + aliased :]
    out, mixed, sem = rest
    conditional = half[0] == 0
    guidance = guide[0]
    at = 0
    for index in range(count):
        own = pieces[index][...].astype(jnp.float32)
        theirs = pieces[count + index][...].astype(jnp.float32)
        cond = jnp.where(conditional, own, theirs)
        uncond = jnp.where(conditional, theirs, own)
        width = own.shape[1]
        mixed[:, at : at + width] = (uncond + guidance * (cond - uncond)).astype(jnp.bfloat16)
        at += width
    copy = pltpu.make_async_copy(mixed, out.at[:, pl.ds(begin, at)], sem)
    copy.start()
    copy.wait()


def body(query_rows, key_rows, value_rows, select, counts, guide_scale):
    shards = lax.axis_size("seq") // 2
    me = lax.axis_index("seq").astype(jnp.int32)
    my_half = (me % 2).reshape(1)
    tokens, row_width = query_rows.shape
    tiles_dev = tokens // TILE
    picks = select.shape[1]
    half_rows = tokens // 2
    dtype = query_rows.dtype
    span = CAP * TILE
    chunks = len(CHUNKS)
    begins = [sum(CHUNKS[:index]) * HEAD_DIM for index in range(chunks)]
    widths = [heads * HEAD_DIM for heads in CHUNKS]

    far = len(OFFSETS) - NEAR

    def box(width):
        return jax.ShapeDtypeStruct((2, span, width), dtype)

    table_size = tiles_dev * (picks + 1) + far * CAP
    table, *packed = pl.pallas_call(
        functools.partial(pack_near_kernel, (tiles_dev, picks, shards)),
        out_shape=[jax.ShapeDtypeStruct((table_size,), jnp.int32)] + [box(row_width)] * NEAR,
        in_specs=[SMEM, SMEM, SMEM, HBM, HBM],
        out_specs=[SMEM] + [HBM] * NEAR,
        scratch_shapes=[
            pltpu.VMEM((2, tokens, row_width), dtype),
            pltpu.SemaphoreType.DMA((2 * tiles_dev,)),
            pltpu.SemaphoreType.DMA((NEAR * CAP * 2,)),
        ],
        name="pack_near",
    )(me.reshape(1), select.T, counts, key_rows, value_rows)
    near = [shifted(piece, "seq", 2 * off) for piece, off in zip(packed, OFFSETS)]
    packed = pl.pallas_call(
        functools.partial(pack_far_kernel, tiles_dev * (picks + 1), begins, widths),
        out_shape=[box(width) for width in widths for _ in range(far)],
        in_specs=[SMEM, VMEM, VMEM],
        out_specs=[VMEM] * (chunks * far),
        compiler_params=PARAMS,
        name="pack_far",
    )(table, key_rows, value_rows)

    landed = []
    for index in range(chunks):
        pieces = packed[far * index : far * (index + 1)]
        landed.append(
            near
            + [shifted(piece, "seq", 2 * off) for piece, off in zip(pieces, OFFSETS[NEAR:])]
        )

    kept_all, their_all = [], []
    for index, (begin, width, heads) in enumerate(zip(begins, widths, CHUNKS)):
        sent, kept = pl.pallas_call(
            functools.partial(attend_kernel, begin, heads, picks),
            out_shape=[jax.ShapeDtypeStruct((half_rows, width), dtype)] * 2,
            in_specs=[SMEM, SMEM] + [VMEM] * 7,
            out_specs=[VMEM, VMEM],
            scratch_shapes=[
                pltpu.VMEM((2, tokens + len(OFFSETS) * span, width), dtype),
                pltpu.VMEM((tokens, width), dtype),
            ],
            compiler_params=PARAMS,
        )(my_half, table, query_rows, key_rows, value_rows, *landed[index])
        kept_all.append(kept)
        their_all.append(partner(sent, "seq"))

    early = chunks - 1
    guided = None
    for first, last in ((0, early), (early, chunks)):
        pieces = kept_all[first:last] + their_all[first:last]
        aliased = [] if guided is None else [guided]
        guided = pl.pallas_call(
            functools.partial(combine_kernel, begins[first], last - first, len(aliased)),
            out_shape=jax.ShapeDtypeStruct((half_rows, row_width), dtype),
            in_specs=[SMEM, SMEM] + [VMEM] * len(pieces) + [HBM] * len(aliased),
            out_specs=HBM,
            scratch_shapes=[
                pltpu.VMEM((half_rows, sum(widths[first:last])), dtype),
                pltpu.SemaphoreType.DMA,
            ],
            input_output_aliases={2 + len(pieces): 0} if aliased else {},
            compiler_params=PARAMS,
        )(my_half, guide_scale, *pieces, *aliased)
    return guided


def solution(mesh):
    in_specs = (
        P(("groups", "seq"), None),
        P(("groups", "seq"), None),
        P(("groups", "seq"), None),
        P("groups", None),
        P("groups"),
        P("groups"),
    )
    out_specs = P(("groups", "seq"), None)

    return jax.shard_map(body, mesh=mesh, in_specs=in_specs, out_specs=out_specs, check_vma=False)
```

```python
import functools

import jax
import jax.numpy as jnp
from jax import lax
from jax.experimental import pallas as pl
from jax.experimental.pallas import tpu as pltpu
from jax.sharding import PartitionSpec as P

HEAD_DIM = 128
TILE = 128
REACH = 2
CAP = 2
OFFSETS = (1, -1, 2, -2)
NEAR = 2
CHUNKS = (8, 4)
GROUP = 4
EXP2_SCALE = HEAD_DIM ** (-0.5) * 1.4426950408889634
VMEM_BYTES = 24 << 20


SMEM = pl.BlockSpec(memory_space=pltpu.SMEM)
VMEM = pl.BlockSpec(memory_space=pltpu.VMEM)
HBM = pl.BlockSpec(memory_space=pltpu.HBM)
PARAMS = pltpu.CompilerParams(vmem_limit_bytes=VMEM_BYTES)


def shifted(block, axis, distance):
    devices = range(lax.axis_size(axis))
    route = [(i - distance, i) for i in devices if i - distance in devices]
    return lax.ppermute(block, axis, route)


def partner(block, axis):
    route = [(i, i ^ 1) for i in range(lax.axis_size(axis))]
    return lax.ppermute(block, axis, route)


def first_bit(bits):
    return jnp.where(
        bits & 1 != 0, 0, jnp.where(bits & 2 != 0, 1, jnp.where(bits & 4 != 0, 2, 3))
    )


def wanted_bits(select, counts, shard, tiles_dev, picks):
    bits = jnp.int32(0)
    base = (shard - REACH) * tiles_dev
    for row in range(tiles_dev):
        line = shard * tiles_dev + row
        live = counts[line]
        for pick in range(picks):
            place = jnp.clip(select[pick, line] - base, 0, (2 * REACH + 1) * tiles_dev - 1)
            bits = bits | jnp.where(pick < live, jnp.left_shift(1, place), 0)
    return bits


def fill_table(my_shard, tiles, select, counts, table, tiles_dev, picks):
    bits = wanted_bits(select, counts, my_shard, tiles_dev, picks)
    for row in range(tiles_dev):
        line = my_shard * tiles_dev + row
        table[tiles_dev * picks + row] = counts[line]
        for pick in range(picks):
            tile = select[pick, line]
            away = jnp.clip(tile // tiles_dev - my_shard, -REACH, REACH)
            within = tile % tiles_dev
            theirs = jnp.right_shift(bits, (away + REACH) * tiles_dev)
            below = theirs & (jnp.left_shift(1, within) - 1)
            rank = (below & 1) + (jnp.right_shift(below, 1) & 1) + (jnp.right_shift(below, 2) & 1)
            rank = jnp.minimum(rank, CAP - 1)
            block = 2 * (jnp.abs(away) - 1) + jnp.where(away < 0, 0, 1)
            slot = jnp.where(away == 0, within, tiles_dev + block * CAP + rank)
            table[row * picks + pick] = slot
    for index, tile in enumerate(tiles):
        table[tiles_dev * (picks + 1) + index] = tile


def sent_tiles(my_shard, offset, select, counts, tiles_dev, picks, shards):
    reader = jnp.clip(my_shard + offset, 0, shards - 1)
    bits = wanted_bits(select, counts, reader, tiles_dev, picks)
    mine = jnp.right_shift(bits, (REACH - offset) * tiles_dev) & 15
    return [first_bit(mine), first_bit(mine & (mine - 1))]


def tile_rows(tile):
    return pl.ds(pl.multiple_of(tile * TILE, TILE), TILE)


def pack_near_kernel(sizes, me, select, counts, keys, values, table, *rest):
    outs, (stage, load_sems, sems) = rest[:NEAR], rest[NEAR:]
    my_shard = me[0] // 2
    loads = []
    for which, rows in enumerate((keys, values)):
        for tile in range(sizes[0]):
            part = pl.ds(tile * TILE, TILE)
            loads.append(
                pltpu.make_async_copy(
                    rows.at[part, :], stage.at[which, part, :], load_sems.at[len(loads)]
                )
            )
    for load in loads:
        load.start()
    near = [sent_tiles(my_shard, off, select, counts, *sizes) for off in OFFSETS[:NEAR]]
    for load in loads:
        load.wait()
    copies = []
    for index, chosen in enumerate(near):
        for slot, tile in enumerate(chosen):
            for which in range(2):
                copy = pltpu.make_async_copy(
                    stage.at[which, tile_rows(tile), :],
                    outs[index].at[which, pl.ds(slot * TILE, TILE), :],
                    sems.at[len(copies)],
                )
                copy.start()
                copies.append(copy)
    tiles = []
    for offset in OFFSETS[NEAR:]:
        tiles += sent_tiles(my_shard, offset, select, counts, *sizes)
    fill_table(my_shard, tiles, select, counts, table, *sizes[:2])
    for copy in copies:
        copy.wait()


def pack_far_kernel(first, begins, widths, table, keys, values, *outs):
    far = len(OFFSETS) - NEAR
    for index, (begin, width) in enumerate(zip(begins, widths)):
        for place in range(far):
            out = outs[index * far + place]
            for slot in range(CAP):
                rows = tile_rows(table[first + place * CAP + slot])
                for which, source in enumerate((keys, values)):
                    out[which, slot * TILE : (slot + 1) * TILE, :] = source[
                        rows, begin : begin + width
                    ]


def attend_tile(query_ref, pool, result, slots, rows, heads):
    cols = [slice(head * HEAD_DIM, (head + 1) * HEAD_DIM) for head in heads]
    scores, weights, totals, mixed = [], [], [], []
    for col in cols:
        keys = jnp.concatenate([pool[0, slot, col] for slot in slots], axis=0)
        scores.append(
            lax.dot_general(
                query_ref[rows, col],
                keys,
                (((1,), (1,)), ((), ())),
                preferred_element_type=jnp.float32,
            )
        )
    tops = [jnp.max(score, axis=1, keepdims=True) for score in scores]
    for score, top in zip(scores, tops):
        weight = jnp.exp2((score - top) * EXP2_SCALE)
        totals.append(jnp.sum(weight, axis=1, keepdims=True))
        weights.append(weight.astype(jnp.bfloat16))
    for weight, col in zip(weights, cols):
        values = jnp.concatenate([pool[1, slot, col] for slot in slots], axis=0)
        mixed.append(jnp.dot(weight, values, preferred_element_type=jnp.float32))
    for mix, total, col in zip(mixed, totals, cols):
        result[rows, col] = (mix / total).astype(jnp.bfloat16)


def warm_kernel(table, queries, out):
    del queries
    for index in range(table.shape[0]):
        out[index] = table[index]


def attend_kernel(begin, heads, picks, half, table, queries, keys, values, *rest):
    lands, (sent, kept, query_ref, pool, result, sems) = rest[:4], rest[4:]
    tokens = queries.shape[0]
    tiles_dev = tokens // TILE
    span = CAP * TILE
    width = heads * HEAD_DIM
    cols = pl.ds(begin, width)
    copies = [
        pltpu.make_async_copy(queries.at[:, cols], query_ref, sems.at[0]),
        pltpu.make_async_copy(keys.at[:, cols], pool.at[0, pl.ds(0, tokens), :], sems.at[1]),
        pltpu.make_async_copy(values.at[:, cols], pool.at[1, pl.ds(0, tokens), :], sems.at[2]),
    ]
    for index, land in enumerate(lands):
        part = cols if index < NEAR else pl.ds(0, width)
        copies.append(
            pltpu.make_async_copy(
                land.at[:, :, part],
                pool.at[:, pl.ds(tokens + index * span, span), :],
                sems.at[3 + index],
            )
        )
    for copy in copies:
        copy.start()
    for copy in copies:
        copy.wait()

    def one_tile(tile, carry):
        rows = tile_rows(tile)
        slots = [tile_rows(table[tile * picks + pick]) for pick in range(picks)]
        live = table[tiles_dev * picks + tile]
        for count in range(2, picks + 1):

            @pl.when(live == count)
            def _(count=count):
                for group in range(0, heads, GROUP):
                    attend_tile(
                        query_ref, pool, result, slots[:count], rows, range(group, group + GROUP)
                    )

        return carry

    lax.fori_loop(0, tiles_dev, one_tile, 0)
    half_rows = tokens // 2
    my_half = half[0]
    sent[...] = result[pl.ds(pl.multiple_of((1 - my_half) * half_rows, half_rows), half_rows), :]
    kept[...] = result[pl.ds(pl.multiple_of(my_half * half_rows, half_rows), half_rows), :]


def combine_kernel(begin, count, aliased, half, guide, *rest):
    pieces, rest = rest[: 2 * count], rest[2 * count + aliased :]
    out, mixed, sem = rest
    conditional = half[0] == 0
    guidance = guide[0]
    at = 0
    for index in range(count):
        own = pieces[index][...].astype(jnp.float32)
        theirs = pieces[count + index][...].astype(jnp.float32)
        cond = jnp.where(conditional, own, theirs)
        uncond = jnp.where(conditional, theirs, own)
        width = own.shape[1]
        mixed[:, at : at + width] = (uncond + guidance * (cond - uncond)).astype(jnp.bfloat16)
        at += width
    copy = pltpu.make_async_copy(mixed, out.at[:, pl.ds(begin, at)], sem)
    copy.start()
    copy.wait()


def body(query_rows, key_rows, value_rows, select, counts, guide_scale):
    shards = lax.axis_size("seq") // 2
    me = lax.axis_index("seq").astype(jnp.int32)
    my_half = (me % 2).reshape(1)
    tokens, row_width = query_rows.shape
    tiles_dev = tokens // TILE
    picks = select.shape[1]
    half_rows = tokens // 2
    dtype = query_rows.dtype
    span = CAP * TILE
    chunks = len(CHUNKS)
    begins = [sum(CHUNKS[:index]) * HEAD_DIM for index in range(chunks)]
    widths = [heads * HEAD_DIM for heads in CHUNKS]

    far = len(OFFSETS) - NEAR

    def box(width):
        return jax.ShapeDtypeStruct((2, span, width), dtype)

    table_size = tiles_dev * (picks + 1) + far * CAP
    table, *packed = pl.pallas_call(
        functools.partial(pack_near_kernel, (tiles_dev, picks, shards)),
        out_shape=[jax.ShapeDtypeStruct((table_size,), jnp.int32)] + [box(row_width)] * NEAR,
        in_specs=[SMEM, SMEM, SMEM, HBM, HBM],
        out_specs=[SMEM] + [HBM] * NEAR,
        scratch_shapes=[
            pltpu.VMEM((2, tokens, row_width), dtype),
            pltpu.SemaphoreType.DMA((2 * tiles_dev,)),
            pltpu.SemaphoreType.DMA((NEAR * CAP * 2,)),
        ],
        name="pack_near",
    )(me.reshape(1), select.T, counts, key_rows, value_rows)
    near = [shifted(piece, "seq", 2 * off) for piece, off in zip(packed, OFFSETS)]
    packed = pl.pallas_call(
        functools.partial(pack_far_kernel, tiles_dev * (picks + 1), begins, widths),
        out_shape=[box(width) for width in widths for _ in range(far)],
        in_specs=[SMEM, VMEM, VMEM],
        out_specs=[VMEM] * (chunks * far),
        compiler_params=PARAMS,
        name="pack_far",
    )(table, key_rows, value_rows)

    landed = []
    for index in range(chunks):
        pieces = packed[far * index : far * (index + 1)]
        landed.append(
            near
            + [shifted(piece, "seq", 2 * off) for piece, off in zip(pieces, OFFSETS[NEAR:])]
        )

    table = pl.pallas_call(
        warm_kernel,
        out_shape=jax.ShapeDtypeStruct(table.shape, table.dtype),
        in_specs=[SMEM, VMEM],
        out_specs=SMEM,
        compiler_params=PARAMS,
        name="warm_queries",
    )(table, query_rows)

    kept_all, their_all = [], []
    for index, (begin, width, heads) in enumerate(zip(begins, widths, CHUNKS)):
        sent, kept = pl.pallas_call(
            functools.partial(attend_kernel, begin, heads, picks),
            out_shape=[jax.ShapeDtypeStruct((half_rows, width), dtype)] * 2,
            in_specs=[SMEM, SMEM] + [HBM] * 7,
            out_specs=[VMEM, VMEM],
            scratch_shapes=[
                pltpu.VMEM((tokens, width), dtype),
                pltpu.VMEM((2, tokens + len(OFFSETS) * span, width), dtype),
                pltpu.VMEM((tokens, width), dtype),
                pltpu.SemaphoreType.DMA((3 + len(OFFSETS),)),
            ],
            compiler_params=PARAMS,
        )(my_half, table, query_rows, key_rows, value_rows, *landed[index])
        kept_all.append(kept)
        their_all.append(partner(sent, "seq"))

    early = chunks - 1
    guided = None
    for first, last in ((0, early), (early, chunks)):
        pieces = kept_all[first:last] + their_all[first:last]
        aliased = [] if guided is None else [guided]
        guided = pl.pallas_call(
            functools.partial(combine_kernel, begins[first], last - first, len(aliased)),
            out_shape=jax.ShapeDtypeStruct((half_rows, row_width), dtype),
            in_specs=[SMEM, SMEM] + [VMEM] * len(pieces) + [HBM] * len(aliased),
            out_specs=HBM,
            scratch_shapes=[
                pltpu.VMEM((half_rows, sum(widths[first:last])), dtype),
                pltpu.SemaphoreType.DMA,
            ],
            input_output_aliases={2 + len(pieces): 0} if aliased else {},
            compiler_params=PARAMS,
        )(my_half, guide_scale, *pieces, *aliased)
    return guided


def solution(mesh):
    in_specs = (
        P(("groups", "seq"), None),
        P(("groups", "seq"), None),
        P(("groups", "seq"), None),
        P("groups", None),
        P("groups"),
        P("groups"),
    )
    out_specs = P(("groups", "seq"), None)

    return jax.shard_map(body, mesh=mesh, in_specs=in_specs, out_specs=out_specs, check_vma=False)
```

```python
import functools

import jax
import jax.numpy as jnp
from jax import lax
from jax.experimental import pallas as pl
from jax.experimental.pallas import tpu as pltpu
from jax.sharding import PartitionSpec as P

HEAD_DIM = 128
TILE = 128
REACH = 2
CAP = 2
OFFSETS = (1, -1, 2, -2)
NEAR = 2
CHUNKS = (8, 4)
GROUP = 4
EXP2_SCALE = HEAD_DIM ** (-0.5) * 1.4426950408889634
VMEM_BYTES = 24 << 20


SMEM = pl.BlockSpec(memory_space=pltpu.SMEM)
VMEM = pl.BlockSpec(memory_space=pltpu.VMEM)
HBM = pl.BlockSpec(memory_space=pltpu.HBM)
PARAMS = pltpu.CompilerParams(vmem_limit_bytes=VMEM_BYTES)


def shifted(block, axis, distance):
    devices = range(lax.axis_size(axis))
    route = [(i - distance, i) for i in devices if i - distance in devices]
    return lax.ppermute(block, axis, route)


def partner(block, axis):
    route = [(i, i ^ 1) for i in range(lax.axis_size(axis))]
    return lax.ppermute(block, axis, route)


def first_bit(bits):
    return jnp.where(
        bits & 1 != 0, 0, jnp.where(bits & 2 != 0, 1, jnp.where(bits & 4 != 0, 2, 3))
    )


def wanted_bits(select, counts, shard, tiles_dev, picks):
    bits = jnp.int32(0)
    base = (shard - REACH) * tiles_dev
    for row in range(tiles_dev):
        line = shard * tiles_dev + row
        live = counts[line]
        for pick in range(picks):
            place = jnp.clip(select[pick, line] - base, 0, (2 * REACH + 1) * tiles_dev - 1)
            bits = bits | jnp.where(pick < live, jnp.left_shift(1, place), 0)
    return bits


def fill_table(my_shard, select, counts, table, tiles_dev, picks):
    bits = wanted_bits(select, counts, my_shard, tiles_dev, picks)
    for row in range(tiles_dev):
        line = my_shard * tiles_dev + row
        table[tiles_dev * picks + row] = counts[line]
        for pick in range(picks):
            tile = select[pick, line]
            away = jnp.clip(tile // tiles_dev - my_shard, -REACH, REACH)
            within = tile % tiles_dev
            theirs = jnp.right_shift(bits, (away + REACH) * tiles_dev)
            below = theirs & (jnp.left_shift(1, within) - 1)
            rank = (below & 1) + (jnp.right_shift(below, 1) & 1) + (jnp.right_shift(below, 2) & 1)
            rank = jnp.minimum(rank, CAP - 1)
            block = 2 * (jnp.abs(away) - 1) + jnp.where(away < 0, 0, 1)
            slot = jnp.where(away == 0, within, tiles_dev + block * CAP + rank)
            table[row * picks + pick] = slot


def sent_tiles(my_shard, offset, select, counts, tiles_dev, picks, shards):
    reader = jnp.clip(my_shard + offset, 0, shards - 1)
    bits = wanted_bits(select, counts, reader, tiles_dev, picks)
    mine = jnp.right_shift(bits, (REACH - offset) * tiles_dev) & 15
    return [first_bit(mine), first_bit(mine & (mine - 1))]


def tile_rows(tile):
    return pl.ds(pl.multiple_of(tile * TILE, TILE), TILE)


def pack_near_kernel(sizes, select, counts, keys, values, *rest):
    outs, (stage, load_sems, sems) = rest[:NEAR], rest[NEAR:]
    my_shard = lax.axis_index("seq") // 2
    loads = []
    for which, rows in enumerate((keys, values)):
        for tile in range(sizes[0]):
            part = pl.ds(tile * TILE, TILE)
            loads.append(
                pltpu.make_async_copy(
                    rows.at[part, :], stage.at[which, part, :], load_sems.at[len(loads)]
                )
            )
    for load in loads:
        load.start()
    near = [sent_tiles(my_shard, off, select, counts, *sizes) for off in OFFSETS[:NEAR]]
    for load in loads:
        load.wait()
    copies = []
    for index, chosen in enumerate(near):
        for slot, tile in enumerate(chosen):
            for which in range(2):
                copy = pltpu.make_async_copy(
                    stage.at[which, tile_rows(tile), :],
                    outs[index].at[which, pl.ds(slot * TILE, TILE), :],
                    sems.at[len(copies)],
                )
                copy.start()
                copies.append(copy)
    for copy in copies:
        copy.wait()


def pack_far_kernel(sizes, begins, widths, select, counts, keys, values, near, table, *outs):
    del near
    my_shard = lax.axis_index("seq") // 2
    chosen = []
    for offset in OFFSETS[NEAR:]:
        chosen.append(sent_tiles(my_shard, offset, select, counts, *sizes))
    for index, (begin, width) in enumerate(zip(begins, widths)):
        for place, tiles in enumerate(chosen):
            out = outs[index * len(chosen) + place]
            for slot, tile in enumerate(tiles):
                for which, source in enumerate((keys, values)):
                    out[which, slot * TILE : (slot + 1) * TILE, :] = source[
                        tile_rows(tile), begin : begin + width
                    ]
    fill_table(my_shard, select, counts, table, *sizes[:2])


def attend_tile(query_ref, pool, result, slots, rows, heads):
    cols = [slice(head * HEAD_DIM, (head + 1) * HEAD_DIM) for head in heads]
    scores, weights, totals, mixed = [], [], [], []
    for col in cols:
        keys = jnp.concatenate([pool[0, slot, col] for slot in slots], axis=0)
        scores.append(
            lax.dot_general(
                query_ref[rows, col],
                keys,
                (((1,), (1,)), ((), ())),
                preferred_element_type=jnp.float32,
            )
        )
    tops = [jnp.max(score, axis=1, keepdims=True) for score in scores]
    for score, top in zip(scores, tops):
        weight = jnp.exp2((score - top) * EXP2_SCALE)
        totals.append(jnp.sum(weight, axis=1, keepdims=True))
        weights.append(weight.astype(jnp.bfloat16))
    for weight, col in zip(weights, cols):
        values = jnp.concatenate([pool[1, slot, col] for slot in slots], axis=0)
        mixed.append(jnp.dot(weight, values, preferred_element_type=jnp.float32))
    for mix, total, col in zip(mixed, totals, cols):
        result[rows, col] = (mix / total).astype(jnp.bfloat16)


def warm_kernel(table, queries, out):
    del queries
    for index in range(table.shape[0]):
        out[index] = table[index]


def attend_kernel(begin, heads, picks, table, queries, keys, values, *rest):
    lands, (sent, kept, query_ref, pool, result, sems) = rest[:4], rest[4:]
    tokens = queries.shape[0]
    tiles_dev = tokens // TILE
    span = CAP * TILE
    width = heads * HEAD_DIM
    cols = pl.ds(begin, width)
    copies = [
        pltpu.make_async_copy(queries.at[:, cols], query_ref, sems.at[0]),
        pltpu.make_async_copy(keys.at[:, cols], pool.at[0, pl.ds(0, tokens), :], sems.at[1]),
        pltpu.make_async_copy(values.at[:, cols], pool.at[1, pl.ds(0, tokens), :], sems.at[2]),
    ]
    for index, land in enumerate(lands):
        part = cols if index < NEAR else pl.ds(0, width)
        copies.append(
            pltpu.make_async_copy(
                land.at[:, :, part],
                pool.at[:, pl.ds(tokens + index * span, span), :],
                sems.at[3 + index],
            )
        )
    for copy in copies:
        copy.start()
    for copy in copies:
        copy.wait()

    def one_tile(tile, carry):
        rows = tile_rows(tile)
        slots = [tile_rows(table[tile * picks + pick]) for pick in range(picks)]
        live = table[tiles_dev * picks + tile]
        for count in range(2, picks + 1):

            @pl.when(live == count)
            def _(count=count):
                for group in range(0, heads, GROUP):
                    attend_tile(
                        query_ref, pool, result, slots[:count], rows, range(group, group + GROUP)
                    )

        return carry

    lax.fori_loop(0, tiles_dev, one_tile, 0)
    half_rows = tokens // 2
    my_half = lax.axis_index("seq") % 2
    sent[...] = result[pl.ds(pl.multiple_of((1 - my_half) * half_rows, half_rows), half_rows), :]
    kept[...] = result[pl.ds(pl.multiple_of(my_half * half_rows, half_rows), half_rows), :]


def combine_kernel(begin, count, aliased, guide, *rest):
    pieces, rest = rest[: 2 * count], rest[2 * count + aliased :]
    out, mixed, sem = rest
    conditional = lax.axis_index("seq") % 2 == 0
    guidance = guide[0]
    at = 0
    for index in range(count):
        own = pieces[index][...].astype(jnp.float32)
        theirs = pieces[count + index][...].astype(jnp.float32)
        cond = jnp.where(conditional, own, theirs)
        uncond = jnp.where(conditional, theirs, own)
        width = own.shape[1]
        mixed[:, at : at + width] = (uncond + guidance * (cond - uncond)).astype(jnp.bfloat16)
        at += width
    copy = pltpu.make_async_copy(mixed, out.at[:, pl.ds(begin, at)], sem)
    copy.start()
    copy.wait()


def body(query_rows, key_rows, value_rows, select, counts, guide_scale):
    shards = lax.axis_size("seq") // 2
    tokens, row_width = query_rows.shape
    tiles_dev = tokens // TILE
    picks = select.shape[1]
    half_rows = tokens // 2
    dtype = query_rows.dtype
    span = CAP * TILE
    chunks = len(CHUNKS)
    begins = [sum(CHUNKS[:index]) * HEAD_DIM for index in range(chunks)]
    widths = [heads * HEAD_DIM for heads in CHUNKS]

    far = len(OFFSETS) - NEAR

    def box(width):
        return jax.ShapeDtypeStruct((2, span, width), dtype)

    sizes = (tiles_dev, picks, shards)
    packed = pl.pallas_call(
        functools.partial(pack_near_kernel, sizes),
        out_shape=[box(row_width)] * NEAR,
        in_specs=[SMEM, SMEM, HBM, HBM],
        out_specs=[HBM] * NEAR,
        scratch_shapes=[
            pltpu.VMEM((2, tokens, row_width), dtype),
            pltpu.SemaphoreType.DMA((2 * tiles_dev,)),
            pltpu.SemaphoreType.DMA((NEAR * CAP * 2,)),
        ],
        name="pack_near",
    )(select.T, counts, key_rows, value_rows)
    near = []
    for piece, offset in zip(packed, OFFSETS):
        near.append(shifted(piece, "seq", 2 * offset))
    table, *packed = pl.pallas_call(
        functools.partial(pack_far_kernel, sizes, begins, widths),
        out_shape=[jax.ShapeDtypeStruct((tiles_dev * (picks + 1),), jnp.int32)]
        + [box(width) for width in widths for _ in range(far)],
        in_specs=[SMEM, SMEM, VMEM, VMEM, HBM],
        out_specs=[SMEM] + [VMEM] * (chunks * far),
        compiler_params=PARAMS,
        name="pack_far",
    )(select.T, counts, key_rows, value_rows, packed[0])

    landed = []
    for index in range(chunks):
        pieces = packed[far * index : far * (index + 1)]
        landed.append(
            near
            + [shifted(piece, "seq", 2 * off) for piece, off in zip(pieces, OFFSETS[NEAR:])]
        )

    table = pl.pallas_call(
        warm_kernel,
        out_shape=jax.ShapeDtypeStruct(table.shape, table.dtype),
        in_specs=[SMEM, VMEM],
        out_specs=SMEM,
        compiler_params=PARAMS,
        name="warm_queries",
    )(table, query_rows)

    kept_all, their_all = [], []
    for index, (begin, width, heads) in enumerate(zip(begins, widths, CHUNKS)):
        sent, kept = pl.pallas_call(
            functools.partial(attend_kernel, begin, heads, picks),
            out_shape=[jax.ShapeDtypeStruct((half_rows, width), dtype)] * 2,
            in_specs=[SMEM] + [HBM] * 7,
            out_specs=[VMEM, VMEM],
            scratch_shapes=[
                pltpu.VMEM((tokens, width), dtype),
                pltpu.VMEM((2, tokens + len(OFFSETS) * span, width), dtype),
                pltpu.VMEM((tokens, width), dtype),
                pltpu.SemaphoreType.DMA((3 + len(OFFSETS),)),
            ],
            compiler_params=PARAMS,
        )(table, query_rows, key_rows, value_rows, *landed[index])
        kept_all.append(kept)
        their_all.append(partner(sent, "seq"))

    early = chunks - 1
    guided = None
    for first, last in ((0, early), (early, chunks)):
        pieces = kept_all[first:last] + their_all[first:last]
        aliased = [] if guided is None else [guided]
        guided = pl.pallas_call(
            functools.partial(combine_kernel, begins[first], last - first, len(aliased)),
            out_shape=jax.ShapeDtypeStruct((half_rows, row_width), dtype),
            in_specs=[SMEM] + [VMEM] * len(pieces) + [HBM] * len(aliased),
            out_specs=HBM,
            scratch_shapes=[
                pltpu.VMEM((half_rows, sum(widths[first:last])), dtype),
                pltpu.SemaphoreType.DMA,
            ],
            input_output_aliases={1 + len(pieces): 0} if aliased else {},
            compiler_params=PARAMS,
        )(guide_scale, *pieces, *aliased)
    return guided


def solution(mesh):
    in_specs = (
        P(("groups", "seq"), None),
        P(("groups", "seq"), None),
        P(("groups", "seq"), None),
        P("groups", None),
        P("groups"),
        P("groups"),
    )
    out_specs = P(("groups", "seq"), None)

    return jax.shard_map(body, mesh=mesh, in_specs=in_specs, out_specs=out_specs, check_vma=False)
```
